32 devices in a mesh: row: 4 (over y, x), col: 8 (over z, core).
Axes of the slice: x: 2, y: 2, z: 4, core: 2. Of those that a mesh axis runs over, the one named last changes fastest.
Arguments:
- left_tiles: bfloat16 [2, 32, 256, 256], P(None, 'row', 'col'), may hold values from 0.02 to 3, as said below
- right_tile_store: bfloat16 [32, 24, 256, 256], P('col', 'row'), may hold values from 0.019897461 to 1
- right_index: int32 [32, 24], P('col', 'row'), may hold values from 0 to 7, as said below
- right_count: int32 [32, 4], P('col', 'row'), may hold values from 1 to 6
Outputs:
- inflated: bfloat16 [2, 32, 256, 256], P(None, 'col', 'row')
The draws below stay inside these ranges and needn't reach their ends.
Inputs may be any that keep to these rules, and one draw needn't show every extreme that they name: `right_index`: for each column block and each row index the 6 slots name distinct contraction blocks; only the first right_count of them are used. `left_tiles`: positive entries.
All inputs are finite; a program needn't handle non-finite values.
Results may differ from the reference program's by a relative error of at most 0.001.
Values may be sent and summed in bfloat16 or wider, within the bound.
No kernel may reach another device: no remote copies, remote signals or barrier semaphores. Data moves between devices by JAX's collectives and lax.ppermute only.
A program may use at most 64 MiB of HBM per device.

```python
import math
import jax
import jax.numpy as jnp
from jax import lax

TILE_EDGE = 256
NR = 2
KR = 8
QR = 6
COLUMN_BLOCK_NUM = 32
KTOT = 32
SLOTS_PER_BLOCK = 24
N_ROW = 4


def draw_left_tiles(key, part):
    shape = (NR, KTOT, TILE_EDGE, TILE_EDGE)
    ramp = 1.0 + 2.0 * jnp.arange(TILE_EDGE, dtype=jnp.float32) / TILE_EDGE
    values = jax.random.uniform(key, shape, jnp.float32, 0.05, 1.0)
    return (values * ramp[None, None, :, None]).astype(jnp.bfloat16)


def draw_right_index(key, part):
    groups = COLUMN_BLOCK_NUM * (KTOT // KR)
    scores = jax.random.randint(key, (groups, KR), 0, 1 << 20) * KR + jnp.arange(KR)[None, :]
    order = jnp.argsort(scores, axis=1)
    return order[:, :QR].reshape(COLUMN_BLOCK_NUM, KTOT // KR * QR).astype(jnp.int32)


def touch_ends(drawn, own_key, least, largest):
    shape = drawn.shape
    index_at = [jax.random.randint(jax.random.fold_in(own_key, axis), (), 0, shape[axis]) for axis in range(len(shape))]
    drawn = drawn.at[tuple(index_at)].set(least)
    longest = shape.index(max(shape))
    index_at[longest] = (index_at[longest] + 1) % shape[longest]
    return drawn.at[tuple(index_at)].set(largest)


def level_of(key, dims, split, smallest, largest):
    gain = 1.0
    for axis_at, parts in split:
        heights = jax.random.uniform(jax.random.fold_in(jax.random.fold_in(key, 6), axis_at), (parts,), jnp.float32, smallest / len(split), largest / len(split))
        gain = gain * jnp.repeat(jnp.exp(heights), dims[axis_at] // parts).reshape((-1,) + (1,) * (len(dims) - 1 - axis_at))
    return gain


def setup_inputs(seed: int = 0) -> dict:
    streams_of = jax.random.split(jax.random.key(seed), 5)
    left_tiles = draw_left_tiles(jax.random.fold_in(streams_of[4], 71), 0)
    right_tile_store = jnp.clip(jnp.exp(math.log(1.0) - 3.9171631 * jax.random.uniform(streams_of[1], (COLUMN_BLOCK_NUM, SLOTS_PER_BLOCK, TILE_EDGE, TILE_EDGE), jnp.float32) ** level_of(streams_of[1], (COLUMN_BLOCK_NUM, SLOTS_PER_BLOCK, TILE_EDGE, TILE_EDGE), ((0, 8), (1, 4)), -0.2, 0.2)), 0.019897461, 1.0).astype(jnp.bfloat16)
    right_index = draw_right_index(jax.random.fold_in(streams_of[4], 71), 0)
    right_count = touch_ends(jax.random.randint(streams_of[3], (COLUMN_BLOCK_NUM, N_ROW), 1, QR + 1), jax.random.fold_in(streams_of[3], 1), 1, QR).astype(jnp.int32)
    return {"left_tiles": left_tiles, "right_tile_store": right_tile_store, "right_index": right_index, "right_count": right_count}


def reference(left_tiles, right_tile_store, right_index, right_count):
    row_grouping = right_count.shape[1]
    slot_total = right_tile_store.shape[1] // row_grouping
    block_count = left_tiles.shape[1] // row_grouping
    window_blocks = left_tiles.shape[0]
    tile_size = left_tiles.shape[2]

    def single_column(inputs):
        tiles, index, counts = inputs
        offsets = (jnp.arange(row_grouping, dtype=jnp.int32) * block_count).astype(jnp.int32)
        global_index = (index.reshape(row_grouping, slot_total).astype(jnp.int32) + offsets[:, None]).astype(jnp.int32)
        picked = jnp.take(left_tiles, global_index.reshape(-1), axis=1)
        live_mask = (jnp.arange(slot_total, dtype=jnp.int32)[None, :] < counts[:, None]).reshape(-1)
        picked = picked * live_mask.astype(left_tiles.dtype)[None, :, None, None]
        picked = picked.reshape(window_blocks, row_grouping, slot_total, tile_size, tile_size)
        grouped_tiles = tiles.reshape(row_grouping, slot_total, tile_size, tile_size)
        partial_value = jnp.einsum("arqmb,rqbn->armn", picked.astype(jnp.float32), grouped_tiles.astype(jnp.float32))
        return jnp.sum(partial_value, axis=1)

    product = lax.map(single_column, (right_tile_store, right_index, right_count))
    squared = product * product
    column_sums = jnp.sum(squared, axis=(1, 2))
    scaled = squared * ((window_blocks * tile_size) / column_sums[:, None, None, :])
    return jnp.transpose(scaled, (1, 0, 2, 3)).astype(jnp.bfloat16)
```

```python
import functools
import jax
import jax.numpy as jnp
from jax import lax
from jax.experimental import pallas as pl
from jax.experimental.pallas import tpu as pltpu
from jax.sharding import PartitionSpec as P


LEVELS = 65280.0
OFFSET = 32640
LOG_STEPS = 256.0
CODE_ROWS = 16
MAX_DIRECT = 8

VMEM = pl.BlockSpec(memory_space=pltpu.VMEM)
SMEM = pl.BlockSpec(memory_space=pltpu.SMEM)


def product_kernel(n_block, n_row, place_ref, index_ref, count_ref, *refs):
    blocks, right_ref = refs[:n_block], refs[n_block]
    own_ref = refs[n_block + 1]
    sent_refs = refs[n_block + 2 : n_block + 1 + n_row]
    left, partial = refs[-2:]
    column_blocks, slots, tile, _ = right_ref.shape
    kept = left.shape[0] - 1
    part = tile // n_row
    row = place_ref[0]
    for at, block in enumerate(blocks):
        rows = block.shape[1]
        start = pl.multiple_of(place_ref[1 + at] * rows, rows)
        left[:kept, pl.ds(start, rows), :] = block[...]
    left[kept] = jnp.zeros(left.shape[1:], left.dtype)
    for j in range(column_blocks):
        total = None
        for q in range(slots):
            picked = jnp.where(q < count_ref[j, 0], index_ref[j, q], kept)
            term = jnp.dot(left[picked], right_ref[j, q], preferred_element_type=jnp.float32)
            total = term if total is None else total + term
        partial[...] = total
        top = jnp.max(total, axis=0, keepdims=True)
        code = jnp.floor(jnp.log2(top) * LOG_STEPS).astype(jnp.int32) + 2
        grow = LEVELS * jnp.exp2(code.astype(jnp.float32) * (-1.0 / LOG_STEPS))
        own_ref[j] = partial[pl.ds(pl.multiple_of(row * part, part), part), :]
        for k in range(1, n_row):
            peer = row ^ k
            value = partial[pl.ds(pl.multiple_of(peer * part, part), part), :]
            coded = (value * grow + 0.5).astype(jnp.int32) - OFFSET
            sent = sent_refs[k - 1]
            sent[j * part : (j + 1) * part, :] = coded.astype(jnp.int16)
            tail = column_blocks * part + j * CODE_ROWS
            sent[tail : tail + CODE_ROWS, :] = jnp.broadcast_to(code, (CODE_ROWS, tile)).astype(jnp.int16)


def reduce_kernel(n_row, has_before, *refs):
    got_refs = refs[: n_row - 1]
    own_ref = refs[n_row - 1]
    before_ref = refs[n_row] if has_before else None
    squared_ref, sums_ref = refs[-2:]
    column_blocks, part, tile = own_ref.shape
    for j in range(column_blocks):
        total = own_ref[j]
        for got in got_refs:
            tail = column_blocks * part + j * CODE_ROWS
            code = got[tail : tail + CODE_ROWS, :].astype(jnp.int32)[:1]
            shrink = jnp.exp2(code.astype(jnp.float32) * (1.0 / LOG_STEPS)) * (1.0 / LEVELS)
            coded = got[j * part : (j + 1) * part, :].astype(jnp.int32) + OFFSET
            total = total + coded.astype(jnp.float32) * shrink
        squared = total * total
        squared_ref[j] = squared
        sums = jnp.sum(squared, axis=0, keepdims=True)
        if has_before:
            sums = sums + before_ref[j : j + 1]
        sums_ref[j : j + 1] = sums


def scale_kernel(windows, n_row, *refs):
    squared_refs = refs[:windows]
    sums_refs = refs[windows : windows + n_row]
    out_ref = refs[-1]
    column_blocks = out_ref.shape[1]
    tile = out_ref.shape[3]
    total = sums_refs[0][...]
    for other in sums_refs[1:]:
        total = total + other[...]
    scale = (windows * tile) / total
    for a in range(windows):
        for j in range(column_blocks):
            out_ref[a, j] = (squared_refs[a][j] * scale[j : j + 1]).astype(out_ref.dtype)


def exchange(x, axis, n, k, flip=False):
    pairs = [(i, i ^ k) for i in range(n)]
    return lax.ppermute(x, axis, pairs[::-1] if flip else pairs)


def shards(n_row, n_col, left_tiles, right, right_index, right_count):
    windows, kept, rows, tile = left_tiles.shape
    column_blocks, slots = right.shape[:2]
    part = tile // n_row
    row = lax.axis_index("row")
    col = lax.axis_index("col")
    direct = n_col <= MAX_DIRECT and n_col & (n_col - 1) == 0

    gathered = []
    if direct:
        mine = [left_tiles[a] for a in range(windows)]
        far = [[None] * n_col for a in range(windows)]
        for a in range(windows):
            far[a][0] = mine[a]
            for k in range(2, n_col, 2):
                far[a][k] = exchange(mine[a], "col", n_col, k, flip=a % 2 == 1)
        for a in range(windows):
            for k in range(0, n_col, 2):
                far[a][k + 1] = exchange(far[a][k], "col", n_col, 1, flip=a % 2 == 1)
            gathered.append(far[a])
        place = jnp.stack([row] + [col ^ k for k in range(n_col)]).astype(jnp.int32)
    else:
        whole = lax.all_gather(left_tiles, "col", axis=2, tiled=True)
        gathered = [[whole[a]] for a in range(windows)]
        place = jnp.stack([row, row * 0]).astype(jnp.int32)

    n_block = len(gathered[0])
    sent_rows = column_blocks * (part + CODE_ROWS)
    multiply = pl.pallas_call(
        functools.partial(product_kernel, n_block, n_row),
        out_shape=[jax.ShapeDtypeStruct((column_blocks, part, tile), jnp.float32)]
        + [jax.ShapeDtypeStruct((sent_rows, tile), jnp.int16)] * (n_row - 1),
        in_specs=[SMEM] * 3 + [VMEM] * (n_block + 1),
        out_specs=[VMEM] * n_row,
        scratch_shapes=[
            pltpu.VMEM((kept + 1, tile, tile), left_tiles.dtype),
            pltpu.VMEM((tile, tile), jnp.float32),
        ],
        cost_estimate=pl.CostEstimate(
            flops=2 * column_blocks * slots * tile**3,
            bytes_accessed=right.size * 2,
            transcendentals=0,
        ),
        name="product",
    )
    add_up = [
        pl.pallas_call(
            functools.partial(reduce_kernel, n_row, a > 0),
            out_shape=[
                jax.ShapeDtypeStruct((column_blocks, part, tile), jnp.float32),
                jax.ShapeDtypeStruct((column_blocks, tile), jnp.float32),
            ],
            in_specs=[VMEM] * (n_row + (a > 0)),
            out_specs=[VMEM] * 2,
            name="reduce",
        )
        for a in range(windows)
    ]
    squared, sums = [], None
    exchanged = []
    for a in range(windows):
        own, *sent = multiply(place, right_index, right_count, *gathered[a], right)
        got = [exchange(x, "row", n_row, k + 1, flip=a % 2 == 1) for k, x in enumerate(sent)]
        exchanged.append((own, got))
    for a in range(windows):
        own, got = exchanged[a]
        square, sums = add_up[a](*got, own, *([sums] if a else []))
        squared.append(square)
    others = [exchange(sums, "row", n_row, k) for k in range(1, n_row)]
    return pl.pallas_call(
        functools.partial(scale_kernel, windows, n_row),
        out_shape=jax.ShapeDtypeStruct((windows, column_blocks, part, tile), jnp.bfloat16),
        in_specs=[VMEM] * (windows + n_row),
        out_specs=VMEM,
        name="scale",
    )(*squared, sums, *others)


def solution(mesh):
    in_specs = (
        P(None, "row", "col", None),
        P("col", "row", None, None),
        P("col", "row"),
        P("col", "row"),
    )
    out_specs = P(None, "col", "row", None)
    body = functools.partial(shards, mesh.shape["row"], mesh.shape["col"])
    return jax.shard_map(body, mesh=mesh, in_specs=in_specs, out_specs=out_specs, check_vma=False)
```

```python
import functools
import jax
import jax.numpy as jnp
from jax import lax
from jax.experimental import pallas as pl
from jax.experimental.pallas import tpu as pltpu
from jax.sharding import PartitionSpec as P


LEVELS = 65280.0
OFFSET = 32640
LOG_STEPS = 256.0
CODE_ROWS = 16
MAX_DIRECT = 8

VMEM = pl.BlockSpec(memory_space=pltpu.VMEM)
SMEM = pl.BlockSpec(memory_space=pltpu.SMEM)


def stage_kernel(right_ref, out_ref, sems):
    copies = [
        pltpu.make_async_copy(right_ref.at[j], out_ref.at[j], sems.at[j])
        for j in range(right_ref.shape[0])
    ]
    for copy in copies:
        copy.start()
    for copy in copies:
        copy.wait()


def product_kernel(n_row, shifts, index_ref, count_ref, *refs):
    n_block = len(shifts)
    blocks, right_ref = refs[:n_block], refs[n_block]
    own_ref = refs[n_block + 1]
    sent_refs = refs[n_block + 2 : n_block + 1 + n_row]
    left, partial = refs[-2:]
    column_blocks, slots, tile, _ = right_ref.shape
    kept = left.shape[0] - 1
    part = tile // n_row
    row = lax.axis_index("row")
    for block, shift in zip(blocks, shifts):
        rows = block.shape[1]
        if n_block == 1:
            left[:kept] = block[...]
        else:
            start = pl.multiple_of((lax.axis_index("col") ^ shift) * rows, rows)
            left[:kept, pl.ds(start, rows), :] = block[...]
    left[kept] = jnp.zeros(left.shape[1:], left.dtype)
    lines = lax.broadcasted_iota(jnp.int32, (CODE_ROWS, tile), 0)
    codes = jnp.zeros((CODE_ROWS, tile), jnp.int32)
    for j in range(column_blocks):
        total = None
        for q in range(slots):
            picked = jnp.where(q < count_ref[j], index_ref[j, q], kept)
            term = jnp.dot(left[picked], right_ref[j, q], preferred_element_type=jnp.float32)
            total = term if total is None else total + term
        partial[...] = total
        top = jnp.max(total, axis=0, keepdims=True)
        code = jnp.floor(jnp.log2(top) * LOG_STEPS).astype(jnp.int32) + 2
        grow = LEVELS * jnp.exp2(code.astype(jnp.float32) * (-1.0 / LOG_STEPS))
        codes = jnp.where(lines == j, code, codes)
        own_ref[j] = partial[pl.ds(pl.multiple_of(row * part, part), part), :]
        for k in range(1, n_row):
            peer = row ^ k
            value = partial[pl.ds(pl.multiple_of(peer * part, part), part), :]
            coded = (value * grow + 0.5).astype(jnp.int32) - OFFSET
            sent_refs[k - 1][j * part : (j + 1) * part, :] = coded.astype(jnp.int16)
    for sent in sent_refs:
        sent[column_blocks * part :, :] = codes.astype(jnp.int16)


def reduce_kernel(n_row, has_before, *refs):
    got_refs = refs[: n_row - 1]
    own_ref = refs[n_row - 1]
    before_ref = refs[n_row] if has_before else None
    squared_ref, sums_ref = refs[-2:]
    column_blocks, part, _ = own_ref.shape
    shrinks = []
    for got in got_refs:
        code = got[column_blocks * part :, :].astype(jnp.int32)
        shrinks.append(jnp.exp2(code.astype(jnp.float32) * (1.0 / LOG_STEPS)) * (1.0 / LEVELS))
    for j in range(column_blocks):
        total = own_ref[j]
        for got, shrink in zip(got_refs, shrinks):
            coded = got[j * part : (j + 1) * part, :].astype(jnp.int32) + OFFSET
            total = total + coded.astype(jnp.float32) * shrink[j : j + 1]
        squared = total * total
        squared_ref[j] = squared
        sums = jnp.sum(squared, axis=0, keepdims=True)
        if has_before:
            sums = sums + before_ref[j : j + 1]
        sums_ref[j : j + 1] = sums


def scale_kernel(windows, n_row, *refs):
    squared_refs = refs[:windows]
    sums_refs = refs[windows : windows + n_row]
    out_ref = refs[-1]
    column_blocks = out_ref.shape[1]
    tile = out_ref.shape[3]
    total = sums_refs[0][...]
    for other in sums_refs[1:]:
        total = total + other[...]
    scale = (windows * tile) / total
    for a in range(windows):
        for j in range(column_blocks):
            out_ref[a, j] = (squared_refs[a][j] * scale[j : j + 1]).astype(out_ref.dtype)


def exchange(x, axis, n, k, flip=False):
    pairs = [(i, i ^ k) for i in range(n)]
    return lax.ppermute(x, axis, pairs[::-1] if flip else pairs)


def limits(mib):
    return pltpu.CompilerParams(vmem_limit_bytes=mib << 20)


def is_direct(n_col):
    return n_col <= MAX_DIRECT and n_col & (n_col - 1) == 0


def shards(n_row, n_col, left_tiles, right, right_index, right_count):
    windows, kept, _, tile = left_tiles.shape
    column_blocks, slots = right.shape[:2]
    part = tile // n_row
    right_count = right_count.reshape(-1)

    if is_direct(n_col):
        shifts = tuple(range(n_col))
        mine = [left_tiles[a] for a in range(windows)]
        gathered = [[None] * n_col for _ in range(windows)]
        for a in range(windows):
            gathered[a][0] = mine[a]
            for k in range(2, n_col, 2):
                gathered[a][k] = exchange(mine[a], "col", n_col, k, flip=a % 2 == 1)
        for a in range(windows):
            for k in range(0, n_col, 2):
                gathered[a][k + 1] = exchange(gathered[a][k], "col", n_col, 1, flip=a % 2 == 1)
    else:
        shifts = (0,)
        whole = lax.all_gather(left_tiles, "col", axis=2, tiled=True)
        gathered = [[whole[a]] for a in range(windows)]

    staged = pl.pallas_call(
        stage_kernel,
        out_shape=jax.ShapeDtypeStruct(right.shape, right.dtype),
        in_specs=[pl.BlockSpec(memory_space=pltpu.HBM)],
        out_specs=VMEM,
        scratch_shapes=[pltpu.SemaphoreType.DMA((column_blocks,))],
        compiler_params=limits(8),
        name="stage",
    )(right)
    sent_rows = column_blocks * part + CODE_ROWS
    multiply = pl.pallas_call(
        functools.partial(product_kernel, n_row, shifts),
        out_shape=[jax.ShapeDtypeStruct((column_blocks, part, tile), jnp.float32)]
        + [jax.ShapeDtypeStruct((sent_rows, tile), jnp.int16)] * (n_row - 1),
        in_specs=[SMEM] * 2 + [VMEM] * (len(shifts) + 1),
        out_specs=[VMEM] * n_row,
        scratch_shapes=[
            pltpu.VMEM((kept + 1, tile, tile), left_tiles.dtype),
            pltpu.VMEM((tile, tile), jnp.float32),
        ],
        cost_estimate=pl.CostEstimate(
            flops=2 * column_blocks * slots * tile**3,
            bytes_accessed=right.size * 2,
            transcendentals=0,
        ),
        compiler_params=limits(16),
        name="product",
    )
    exchanged = []
    for a in range(windows):
        own, *sent = multiply(right_index, right_count, *gathered[a], staged)
        got = [exchange(x, "row", n_row, k + 1, flip=a % 2 == 1) for k, x in enumerate(sent)]
        exchanged.append((own, got))
    squared, sums = [], None
    for a in range(windows):
        own, got = exchanged[a]
        square, sums = pl.pallas_call(
            functools.partial(reduce_kernel, n_row, a > 0),
            out_shape=[
                jax.ShapeDtypeStruct((column_blocks, part, tile), jnp.float32),
                jax.ShapeDtypeStruct((column_blocks, tile), jnp.float32),
            ],
            in_specs=[VMEM] * (n_row + (a > 0)),
            out_specs=[VMEM] * 2,
            compiler_params=limits(8),
            name="reduce",
        )(*got, own, *([sums] if a else []))
        squared.append(square)
    others = [exchange(sums, "row", n_row, k) for k in range(1, n_row)]
    return pl.pallas_call(
        functools.partial(scale_kernel, windows, n_row),
        out_shape=jax.ShapeDtypeStruct((windows, column_blocks, part, tile), jnp.bfloat16),
        in_specs=[VMEM] * (windows + n_row),
        out_specs=VMEM,
        compiler_params=limits(8),
        name="scale",
    )(*squared, sums, *others)


def solution(mesh):
    in_specs = (
        P(None, "row", "col", None),
        P("col", "row", None, None),
        P("col", "row"),
        P("col", "row"),
    )
    out_specs = P(None, "col", "row", None)
    n_row, n_col = mesh.shape["row"], mesh.shape["col"]

    def body(*args):
        return shards(n_row, n_col, *args)

    return jax.shard_map(body, mesh=mesh, in_specs=in_specs, out_specs=out_specs, check_vma=False)
```

```python
import functools
import jax
import jax.numpy as jnp
from jax import lax
from jax.experimental import pallas as pl
from jax.experimental.pallas import tpu as pltpu
from jax.sharding import PartitionSpec as P


LEVELS = 65280.0
OFFSET = 32640
LOG_STEPS = 256.0
CODE_ROWS = 16

VMEM = pl.BlockSpec(memory_space=pltpu.VMEM)
SMEM = pl.BlockSpec(memory_space=pltpu.SMEM)


def stage_kernel(right_ref, out_ref, sems):
    copies = [
        pltpu.make_async_copy(right_ref.at[j], out_ref.at[j], sems.at[j])
        for j in range(right_ref.shape[0])
    ]
    for copy in copies:
        copy.start()
    for copy in copies:
        copy.wait()


def product_kernel(n_row, window, shifts, index_ref, count_ref, *refs):
    n_block = len(shifts)
    blocks, right_ref = refs[:n_block], refs[n_block]
    own_ref = refs[n_block + 1]
    sent_refs = refs[n_block + 2 : n_block + 1 + n_row]
    left, partial = refs[-2:]
    column_blocks, slots, tile, _ = right_ref.shape
    kept = left.shape[0] - 1
    part = tile // n_row
    row = lax.axis_index("row")
    for block, (shift, ends) in zip(blocks, shifts):
        if block.ndim == 4:
            block = block.at[window]
        rows = block.shape[1]
        if rows == tile:
            left[:kept] = block[...]
            continue
        col = lax.axis_index("col")
        start = pl.multiple_of((col ^ shift) * rows, rows)

        def place(block=block, start=start, rows=rows):
            left[:kept, pl.ds(start, rows), :] = block[...]

        if ends is None:
            place()
        else:
            pl.when(is_end(col, tile // rows) == ends)(place)
    left[kept] = jnp.zeros(left.shape[1:], left.dtype)
    lines = lax.broadcasted_iota(jnp.int32, (CODE_ROWS, tile), 0)
    codes = jnp.zeros((CODE_ROWS, tile), jnp.int32)
    for j in range(column_blocks):
        total = None
        for q in range(slots):
            picked = jnp.where(q < count_ref[j], index_ref[j, q], kept)
            term = jnp.dot(left[picked], right_ref[j, q], preferred_element_type=jnp.float32)
            total = term if total is None else total + term
        partial[...] = total
        top = jnp.max(total, axis=0, keepdims=True)
        code = jnp.floor(jnp.log2(top) * LOG_STEPS).astype(jnp.int32) + 2
        grow = LEVELS * jnp.exp2(code.astype(jnp.float32) * (-1.0 / LOG_STEPS))
        codes = jnp.where(lines == j, code, codes)
        own_ref[j] = partial[pl.ds(pl.multiple_of(row * part, part), part), :]
        for k in range(1, n_row):
            peer = row ^ k
            value = partial[pl.ds(pl.multiple_of(peer * part, part), part), :]
            coded = (value * grow + 0.5).astype(jnp.int32) - OFFSET
            sent_refs[k - 1][j * part : (j + 1) * part, :] = coded.astype(jnp.int16)
    for sent in sent_refs:
        sent[column_blocks * part :, :] = codes.astype(jnp.int16)


def reduce_kernel(n_row, has_before, *refs):
    got_refs = refs[: n_row - 1]
    own_ref = refs[n_row - 1]
    before_ref = refs[n_row] if has_before else None
    squared_ref, sums_ref = refs[-2:]
    column_blocks, part, _ = own_ref.shape
    shrinks = []
    for got in got_refs:
        code = got[column_blocks * part :, :].astype(jnp.int32)
        shrinks.append(jnp.exp2(code.astype(jnp.float32) * (1.0 / LOG_STEPS)) * (1.0 / LEVELS))
    for j in range(column_blocks):
        total = own_ref[j]
        for got, shrink in zip(got_refs, shrinks):
            coded = got[j * part : (j + 1) * part, :].astype(jnp.int32) + OFFSET
            total = total + coded.astype(jnp.float32) * shrink[j : j + 1]
        squared = total * total
        squared_ref[j] = squared
        sums = jnp.sum(squared, axis=0, keepdims=True)
        if has_before:
            sums = sums + before_ref[j : j + 1]
        sums_ref[j : j + 1] = sums


def scale_kernel(windows, n_row, *refs):
    squared_refs = refs[:windows]
    sums_refs = refs[windows : windows + n_row]
    out_ref = refs[-1]
    column_blocks = out_ref.shape[1]
    tile = out_ref.shape[3]
    total = sums_refs[0][...]
    for other in sums_refs[1:]:
        total = total + other[...]
    scale = (windows * tile) / total
    for a in range(windows):
        for j in range(column_blocks):
            out_ref[a, j] = (squared_refs[a][j] * scale[j : j + 1]).astype(out_ref.dtype)


def exchange(x, axis, n, k, flip=False):
    pairs = [(i, i ^ k) for i in range(n)]
    return lax.ppermute(x, axis, pairs[::-1] if flip else pairs)


def limits(mib):
    return pltpu.CompilerParams(vmem_limit_bytes=mib << 20)


def is_end(col, n_col):
    return (col < 2) | (col >= n_col - 2)


def pairs_of(moves):
    return [(2 * i + c, 2 * j + c) for i, j in moves for c in (0, 1)]


def is_direct(n_col):
    return n_col == 8


def shards(n_row, n_col, left_tiles, right, right_index, right_count):
    windows, kept, _, tile = left_tiles.shape
    column_blocks, slots = right.shape[:2]
    part = tile // n_row
    right_count = right_count.reshape(-1)

    if is_direct(n_col):
        swap = [(i, i ^ 1) for i in range(n_col)]
        ends = [p for p in swap if p[0] < 2 or p[0] >= n_col - 2]
        inner = [p for p in swap if p not in ends]
        halves = [left_tiles[0]]
        halves += [x[a] for a, x in [(1, lax.optimization_barrier(left_tiles))]]
        far, middle, gathered = [], [], []
        for a in range(windows):
            flip = -1 if a % 2 else 1
            far.append(lax.ppermute(halves[a], "col", [(i, i ^ 4) for i in range(n_col)][::flip]))
            middle.append(lax.ppermute(halves[a], "col", pairs_of([(1, 2), (2, 1)])[::flip]))
        beside = lax.ppermute(left_tiles, "col", [(i, i ^ 2) for i in range(n_col)])
        pair = lax.ppermute(left_tiles, "col", swap)
        beside_pair = lax.ppermute(beside, "col", swap[::-1])
        shifts = ((0, None), (1, None), (2, None), (3, None), (4, None), (5, None))
        shifts += ((6, False), (7, False), (6, True), (7, True))
        for a in range(windows):
            flip = -1 if a % 2 else 1
            relay = lax.ppermute(far[a], "col", pairs_of([(1, 0), (2, 3)])[::flip])
            blocks = [left_tiles, pair, beside, beside_pair, far[a]]
            blocks.append(lax.ppermute(far[a], "col", swap[::flip]))
            blocks += [middle[a], lax.ppermute(middle[a], "col", inner[::flip])]
            blocks += [relay, lax.ppermute(relay, "col", ends[::flip])]
            gathered.append(blocks)
    else:
        shifts = ((0, None),)
        whole = lax.all_gather(left_tiles, "col", axis=2, tiled=True)
        gathered = [[whole]] * windows

    staged = pl.pallas_call(
        stage_kernel,
        out_shape=jax.ShapeDtypeStruct(right.shape, right.dtype),
        in_specs=[pl.BlockSpec(memory_space=pltpu.HBM)],
        out_specs=VMEM,
        scratch_shapes=[pltpu.SemaphoreType.DMA((column_blocks,))],
        compiler_params=limits(8),
        name="stage",
    )(right)
    sent_rows = column_blocks * part + CODE_ROWS
    multiply = lambda a: pl.pallas_call(
        functools.partial(product_kernel, n_row, a, shifts),
        out_shape=[jax.ShapeDtypeStruct((column_blocks, part, tile), jnp.float32)]
        + [jax.ShapeDtypeStruct((sent_rows, tile), jnp.int16)] * (n_row - 1),
        in_specs=[SMEM] * 2 + [VMEM] * (len(shifts) + 1),
        out_specs=[VMEM] * n_row,
        scratch_shapes=[
            pltpu.VMEM((kept + 1, tile, tile), left_tiles.dtype),
            pltpu.VMEM((tile, tile), jnp.float32),
        ],
        cost_estimate=pl.CostEstimate(
            flops=2 * column_blocks * slots * tile**3,
            bytes_accessed=right.size * 2,
            transcendentals=0,
        ),
        compiler_params=limits(16),
        name="product",
    )
    exchanged = []
    for a in range(windows):
        own, *sent = multiply(a)(right_index, right_count, *gathered[a], staged)
        got = [exchange(x, "row", n_row, k + 1, flip=a % 2 == 1) for k, x in enumerate(sent)]
        exchanged.append((own, got))
    squared, sums = [], None
    for a in range(windows):
        own, got = exchanged[a]
        square, sums = pl.pallas_call(
            functools.partial(reduce_kernel, n_row, a > 0),
            out_shape=[
                jax.ShapeDtypeStruct((column_blocks, part, tile), jnp.float32),
                jax.ShapeDtypeStruct((column_blocks, tile), jnp.float32),
            ],
            in_specs=[VMEM] * (n_row + (a > 0)),
            out_specs=[VMEM] * 2,
            compiler_params=limits(8),
            name="reduce",
        )(*got, own, *([sums] if a else []))
        squared.append(square)
    others = [exchange(sums, "row", n_row, k) for k in range(1, n_row)]
    return pl.pallas_call(
        functools.partial(scale_kernel, windows, n_row),
        out_shape=jax.ShapeDtypeStruct((windows, column_blocks, part, tile), jnp.bfloat16),
        in_specs=[VMEM] * (windows + n_row),
        out_specs=VMEM,
        compiler_params=limits(8),
        name="scale",
    )(*squared, sums, *others)


def solution(mesh):
    in_specs = (
        P(None, "row", "col", None),
        P("col", "row", None, None),
        P("col", "row"),
        P("col", "row"),
    )
    out_specs = P(None, "col", "row", None)
    n_row, n_col = mesh.shape["row"], mesh.shape["col"]

    def body(*args):
        return shards(n_row, n_col, *args)

    return jax.shard_map(body, mesh=mesh, in_specs=in_specs, out_specs=out_specs, check_vma=False)
```

```python
import functools
import jax
import jax.numpy as jnp
from jax import lax
from jax.experimental import pallas as pl
from jax.experimental.pallas import tpu as pltpu
from jax.sharding import PartitionSpec as P


LEVELS = 65280.0
OFFSET = 32640
LOG_STEPS = 256.0
CODE_ROWS = 16
LINE = 4

VMEM = pl.BlockSpec(memory_space=pltpu.VMEM)
SMEM = pl.BlockSpec(memory_space=pltpu.SMEM)


def stage_kernel(right_ref, out_ref, sems):
    copies = [
        pltpu.make_async_copy(right_ref.at[j], out_ref.at[j], sems.at[j])
        for j in range(right_ref.shape[0])
    ]
    for copy in copies:
        copy.start()
    for copy in copies:
        copy.wait()


def join_kernel(mine_ref, other_ref, *out_refs):
    rows = mine_ref.shape[2]
    core = lax.axis_index("col") & 1
    for a, out_ref in enumerate(out_refs):
        out_ref[:, pl.ds(pl.multiple_of(core * rows, rows), rows), :] = mine_ref[a]
        out_ref[:, pl.ds(pl.multiple_of((1 - core) * rows, rows), rows), :] = other_ref[a]


def product_kernel(n_row, steps, index_ref, count_ref, *refs):
    n_block = len(steps)
    blocks, right_ref = refs[:n_block], refs[n_block]
    own_ref = refs[n_block + 1]
    sent_refs = refs[n_block + 2 : n_block + 1 + n_row]
    left, partial = refs[-2:]
    column_blocks, slots, tile, _ = right_ref.shape
    kept = left.shape[0] - 1
    part = tile // n_row
    row = lax.axis_index("row")
    for block, step in zip(blocks, steps):
        rows = block.shape[1]
        if rows == tile:
            left[:kept] = block[...]
            continue
        col = lax.axis_index("col")
        source = (col >> 1) + (2 * (col & 1) - 1) * step

        def place(block=block, source=source, rows=rows):
            left[:kept, pl.ds(pl.multiple_of(source * rows, rows), rows), :] = block[...]

        if step:
            pl.when((source >= 0) & (source < tile // rows))(place)
        else:
            place()
    left[kept] = jnp.zeros(left.shape[1:], left.dtype)
    lines = lax.broadcasted_iota(jnp.int32, (CODE_ROWS, tile), 0)
    codes = jnp.zeros((CODE_ROWS, tile), jnp.int32)
    for j in range(column_blocks):
        total = None
        for q in range(slots):
            picked = jnp.where(q < count_ref[j], index_ref[j, q], kept)
            term = jnp.dot(left[picked], right_ref[j, q], preferred_element_type=jnp.float32)
            total = term if total is None else total + term
        partial[...] = total
        top = jnp.max(total, axis=0, keepdims=True)
        code = jnp.floor(jnp.log2(top) * LOG_STEPS).astype(jnp.int32) + 2
        grow = LEVELS * jnp.exp2(code.astype(jnp.float32) * (-1.0 / LOG_STEPS))
        codes = jnp.where(lines == j, code, codes)
        own_ref[j] = partial[pl.ds(pl.multiple_of(row * part, part), part), :]
        for k in range(1, n_row):
            peer = row ^ k
            value = partial[pl.ds(pl.multiple_of(peer * part, part), part), :]
            coded = (value * grow + 0.5).astype(jnp.int32) - OFFSET
            sent_refs[k - 1][j * part : (j + 1) * part, :] = coded.astype(jnp.int16)
    for sent in sent_refs:
        sent[column_blocks * part :, :] = codes.astype(jnp.int16)


def reduce_kernel(n_row, has_before, *refs):
    got_refs = refs[: n_row - 1]
    own_ref = refs[n_row - 1]
    before_ref = refs[n_row] if has_before else None
    squared_ref, sums_ref = refs[-2:]
    column_blocks, part, _ = own_ref.shape
    shrinks = []
    for got in got_refs:
        code = got[column_blocks * part :, :].astype(jnp.int32)
        shrinks.append(jnp.exp2(code.astype(jnp.float32) * (1.0 / LOG_STEPS)) * (1.0 / LEVELS))
    for j in range(column_blocks):
        total = own_ref[j]
        for got, shrink in zip(got_refs, shrinks):
            coded = got[j * part : (j + 1) * part, :].astype(jnp.int32) + OFFSET
            total = total + coded.astype(jnp.float32) * shrink[j : j + 1]
        squared = total * total
        squared_ref[j] = squared
        sums = jnp.sum(squared, axis=0, keepdims=True)
        if has_before:
            sums = sums + before_ref[j : j + 1]
        sums_ref[j : j + 1] = sums


def scale_kernel(windows, n_row, *refs):
    squared_refs = refs[:windows]
    sums_refs = refs[windows : windows + n_row]
    out_ref = refs[-1]
    column_blocks = out_ref.shape[1]
    tile = out_ref.shape[3]
    total = sums_refs[0][...]
    for other in sums_refs[1:]:
        total = total + other[...]
    scale = (windows * tile) / total
    for a in range(windows):
        for j in range(column_blocks):
            out_ref[a, j] = (squared_refs[a][j] * scale[j : j + 1]).astype(out_ref.dtype)


def exchange(x, axis, n, k, flip=False):
    pairs = [(i, i ^ k) for i in range(n)]
    return lax.ppermute(x, axis, pairs[::-1] if flip else pairs)


def limits(mib):
    return pltpu.CompilerParams(vmem_limit_bytes=mib << 20)


def is_line(n_col):
    return n_col == 2 * LINE


def both_ways(moves):
    up = [(2 * i, 2 * j) for i, j in moves]
    return up + [(2 * LINE - 1 - i, 2 * LINE - 1 - j) for i, j in up]


def shards(n_row, n_col, left_tiles, right, right_index, right_count):
    windows, kept, rows, tile = left_tiles.shape
    column_blocks, slots = right.shape[:2]
    part = tile // n_row
    right_count = right_count.reshape(-1)

    if is_line(n_col):
        swap = [(i, i ^ 1) for i in range(n_col)]
        pair = lax.ppermute(left_tiles, "col", swap)
        joined = pl.pallas_call(
            join_kernel,
            out_shape=[jax.ShapeDtypeStruct((kept, 2 * rows, tile), left_tiles.dtype)] * windows,
            in_specs=[VMEM] * 2,
            out_specs=[VMEM] * windows,
            compiler_params=limits(8),
            name="join",
        )(left_tiles, pair)
        first = both_ways([(i, i + 1) for i in range(LINE - 1)])
        second = both_ways([(i, i + 1) for i in range(1, LINE - 1)])
        third = both_ways([(1, LINE - 1)])
        steps = (0, 1, -1, 2, -2, 3, -3)
        gathered = []
        for a in range(windows):
            flip = -1 if a % 2 else 1
            one = lax.ppermute(joined[a], "col", first[::flip])
            two = lax.ppermute(one, "col", second[::flip])
            three = lax.ppermute(one, "col", third[::flip])
            blocks = [joined[a]]
            for x in (one, two, three):
                blocks += [x, lax.ppermute(x, "col", swap[::flip])]
            gathered.append(blocks)
    else:
        steps = (0,)
        whole = lax.all_gather(left_tiles, "col", axis=2, tiled=True)
        gathered = [[whole[a]] for a in range(windows)]

    staged = pl.pallas_call(
        stage_kernel,
        out_shape=jax.ShapeDtypeStruct(right.shape, right.dtype),
        in_specs=[pl.BlockSpec(memory_space=pltpu.HBM)],
        out_specs=VMEM,
        scratch_shapes=[pltpu.SemaphoreType.DMA((column_blocks,))],
        compiler_params=limits(8),
        name="stage",
    )(right)
    sent_rows = column_blocks * part + CODE_ROWS
    multiply = pl.pallas_call(
        functools.partial(product_kernel, n_row, steps),
        out_shape=[jax.ShapeDtypeStruct((column_blocks, part, tile), jnp.float32)]
        + [jax.ShapeDtypeStruct((sent_rows, tile), jnp.int16)] * (n_row - 1),
        in_specs=[SMEM] * 2 + [VMEM] * (len(steps) + 1),
        out_specs=[VMEM] * n_row,
        scratch_shapes=[
            pltpu.VMEM((kept + 1, tile, tile), left_tiles.dtype),
            pltpu.VMEM((tile, tile), jnp.float32),
        ],
        cost_estimate=pl.CostEstimate(
            flops=2 * column_blocks * slots * tile**3,
            bytes_accessed=right.size * 2,
            transcendentals=0,
        ),
        compiler_params=limits(16),
        name="product",
    )
    exchanged = []
    for a in range(windows):
        own, *sent = multiply(right_index, right_count, *gathered[a], staged)
        got = [exchange(x, "row", n_row, k + 1, flip=a % 2 == 1) for k, x in enumerate(sent)]
        exchanged.append((own, got))
    squared, sums = [], None
    for a in range(windows):
        own, got = exchanged[a]
        square, sums = pl.pallas_call(
            functools.partial(reduce_kernel, n_row, a > 0),
            out_shape=[
                jax.ShapeDtypeStruct((column_blocks, part, tile), jnp.float32),
                jax.ShapeDtypeStruct((column_blocks, tile), jnp.float32),
            ],
            in_specs=[VMEM] * (n_row + (a > 0)),
            out_specs=[VMEM] * 2,
            compiler_params=limits(8),
            name="reduce",
        )(*got, own, *([sums] if a else []))
        squared.append(square)
    others = [exchange(sums, "row", n_row, k) for k in range(1, n_row)]
    return pl.pallas_call(
        functools.partial(scale_kernel, windows, n_row),
        out_shape=jax.ShapeDtypeStruct((windows, column_blocks, part, tile), jnp.bfloat16),
        in_specs=[VMEM] * (windows + n_row),
        out_specs=VMEM,
        compiler_params=limits(8),
        name="scale",
    )(*squared, sums, *others)


def solution(mesh):
    in_specs = (
        P(None, "row", "col", None),
        P("col", "row", None, None),
        P("col", "row"),
        P("col", "row"),
    )
    out_specs = P(None, "col", "row", None)
    n_row, n_col = mesh.shape["row"], mesh.shape["col"]

    def body(*args):
        return shards(n_row, n_col, *args)

    return jax.shard_map(body, mesh=mesh, in_specs=in_specs, out_specs=out_specs, check_vma=False)
```

```python
import functools
import jax
import jax.numpy as jnp
from jax import lax
from jax.experimental import pallas as pl
from jax.experimental.pallas import tpu as pltpu
from jax.sharding import PartitionSpec as P


LEVELS = 65280.0
OFFSET = 32640
LOG_STEPS = 256.0
CODE_ROWS = 16
LINE = 4

VMEM = pl.BlockSpec(memory_space=pltpu.VMEM)
SMEM = pl.BlockSpec(memory_space=pltpu.SMEM)


def stage_kernel(right_ref, out_ref, sems):
    copies = [
        pltpu.make_async_copy(right_ref.at[j], out_ref.at[j], sems.at[j])
        for j in range(right_ref.shape[0])
    ]
    for copy in copies:
        copy.start()
    for copy in copies:
        copy.wait()


def far_half(half):
    chip = lax.axis_index("col") >> 1
    return jnp.where(lax.axis_index("row") == chip ^ (LINE - 1), 1 - half, half)


def turned(k, half):
    if half is None or k > 2:
        return k
    return jnp.where(lax.axis_index("col") & 1 == 0, k, 3 - k)


def product_kernel(n_row, spans, half, index_ref, count_ref, *refs):
    n_block = len(refs) - n_row - 3
    blocks, right_ref, own_ref = refs[:n_block], refs[n_block], refs[n_block + 1]
    sent_refs = refs[n_block + 2 : n_block + 1 + n_row]
    left, partial = refs[-2:]
    column_blocks, slots, tile, _ = right_ref.shape
    kept, height = left.shape[0] - 1, left.shape[1]
    part = height // n_row // len(spans[0])
    row = lax.axis_index("row")

    def rows_of(owner, at):
        return pl.ds(pl.multiple_of((at * n_row + owner) * part, part), part)

    def block_of(span):
        at, a = span
        return blocks[at] if a is None else blocks[at].at[a]

    if half is None:
        left[:kept] = block_of(spans[0][0])[...]
    else:
        core, chip = lax.axis_index("col") & 1, lax.axis_index("col") >> 1
        ends = (chip == 0) | (chip == LINE - 1)
        first, last = core == 0, core == 1
        placed = [(half, 0, first), (1 - half, 0, last)]
        placed += [(2 + half, 1, first), (3 - half, 1, last), (4, 2, first), (5, 2, last)]
        if half:
            inner = jnp.logical_not(ends)
            placed += [(5, 3, first & inner), (4, 3, last & inner)]
            placed += [(7, 3, first & ends), (6, 3, last & ends)]
        else:
            placed += [(5, 3, first), (4, 3, last)]
        for role, k, wanted in placed:

            def fill(role=role, k=k):
                for at, span in enumerate(spans[role]):
                    left[:kept, rows_of(chip ^ k, at), :] = block_of(span)[...]

            pl.when(wanted)(fill)
    left[kept] = jnp.zeros(left.shape[1:], left.dtype)
    lines = lax.broadcasted_iota(jnp.int32, (CODE_ROWS, tile), 0)
    codes = jnp.zeros((CODE_ROWS, tile), jnp.int32)
    count = len(spans[0])
    for j in range(column_blocks):
        total = None
        for q in range(slots):
            picked = jnp.where(q < count_ref[j], index_ref[j, q], kept)
            term = jnp.dot(left[picked], right_ref[j, q], preferred_element_type=jnp.float32)
            total = term if total is None else total + term
        partial[...] = total
        top = jnp.max(total, axis=0, keepdims=True)
        code = jnp.floor(jnp.log2(top) * LOG_STEPS).astype(jnp.int32) + 2
        grow = LEVELS * jnp.exp2(code.astype(jnp.float32) * (-1.0 / LOG_STEPS))
        codes = jnp.where(lines == j, code, codes)
        for at in range(count):
            own_ref[j, at * part : (at + 1) * part, :] = partial[rows_of(row, at), :]
            for k in range(1, n_row):
                coded = (partial[rows_of(row ^ turned(k, half), at), :] * grow + 0.5).astype(jnp.int32) - OFFSET
                first = (j * count + at) * part
                sent_refs[k - 1][first : first + part, :] = coded.astype(jnp.int16)
    for sent in sent_refs:
        sent[column_blocks * count * part :, :] = codes.astype(jnp.int16)


def reduce_kernel(n_row, has_before, *refs):
    got_refs = refs[: n_row - 1]
    own_ref = refs[n_row - 1]
    before_ref = refs[n_row] if has_before else None
    squared_ref, sums_ref = refs[-2:]
    column_blocks, part, _ = own_ref.shape
    shrinks = []
    for got in got_refs:
        code = got[column_blocks * part :, :].astype(jnp.int32)
        shrinks.append(jnp.exp2(code.astype(jnp.float32) * (1.0 / LOG_STEPS)) * (1.0 / LEVELS))
    for j in range(column_blocks):
        total = own_ref[j]
        for got, shrink in zip(got_refs, shrinks):
            coded = got[j * part : (j + 1) * part, :].astype(jnp.int32) + OFFSET
            total = total + coded.astype(jnp.float32) * shrink[j : j + 1]
        squared = total * total
        squared_ref[j] = squared
        sums = jnp.sum(squared, axis=0, keepdims=True)
        if has_before:
            sums = sums + before_ref[j : j + 1]
        sums_ref[j : j + 1] = sums


def scale_kernel(chunks, n_row, *refs):
    squared_refs = refs[: len(chunks)]
    sums_refs = refs[len(chunks) : len(chunks) + n_row]
    out_ref = refs[-1]
    windows, column_blocks, _, tile = out_ref.shape
    total = sums_refs[0][...]
    for other in sums_refs[1:]:
        total = total + other[...]
    scale = (windows * tile) / total
    for (picked, half), squared in zip(chunks, squared_refs):
        rows = squared.shape[1] // len(picked)
        for at, a in enumerate(picked):
            for j in range(column_blocks):
                value = squared[j, at * rows : (at + 1) * rows, :] * scale[j : j + 1]
                first = 0 if half is None else pl.multiple_of(far_half(half) * rows, rows)
                out_ref[a, j, pl.ds(first, rows), :] = value.astype(out_ref.dtype)


def move(x, axis, pairs, turn=0):
    return lax.ppermute(x, axis, pairs[turn:] + pairs[:turn])


def row_pairs(n_row, n_col, k, half):
    pairs = []
    for i in range(n_row * n_col):
        row, col = i // n_col, i % n_col
        peer = 3 - k if half is not None and k < 3 and col & 1 else k
        pairs.append((i, (row ^ peer) * n_col + col))
    return pairs


def limits(mib):
    return pltpu.CompilerParams(vmem_limit_bytes=mib << 20)


def is_line(n_row, n_col):
    return n_row == LINE and n_col == 2 * LINE


def gather_line(left_tiles, n_col):
    windows = left_tiles.shape[0]
    swap = [(i, i ^ 1) for i in range(n_col)]
    across = [(i, i ^ (4 if i & 1 == 0 else 6)) for i in range(n_col)]
    inner = [p if p[0] & 1 == 0 or 2 <= p[0] < n_col - 2 else (p[0], p[0]) for p in across]
    beside = move(left_tiles, "col", [(i, i ^ 2) for i in range(n_col)])
    own = move(left_tiles, "col", across)
    pair = move(left_tiles, "col", swap, 1)
    other = move(pair, "col", inner)
    relay = move(own, "col", [(2, 1), (n_col - 4, n_col - 1)])
    near_beside = move(beside, "col", swap, 2)
    near_own = move(own, "col", swap, 3)
    near_other = move(other, "col", swap, 4)
    near_relay = move(relay, "col", swap, 5)
    base = [left_tiles, pair, beside, near_beside]
    chunks, gathered = [], []
    for half, more in enumerate(([own, near_own], [other, near_other, relay, near_relay])):
        arrays = base + more
        chunks.append((tuple(range(windows)), half))
        gathered.append((arrays, tuple(tuple((at, a) for a in range(windows)) for at in range(len(arrays)))))
    return chunks, gathered


def shards(n_row, n_col, left_tiles, right, right_index, right_count):
    windows, kept, _, tile = left_tiles.shape
    column_blocks, slots = right.shape[:2]
    right_count = right_count.reshape(-1)

    if is_line(n_row, n_col):
        chunks, gathered = gather_line(left_tiles, n_col)
        height = tile // 2
    else:
        whole = lax.all_gather(left_tiles, "col", axis=2, tiled=True)
        chunks = [((a,), None) for a in range(windows)]
        gathered = [([whole], (((0, a),),)) for a in range(windows)]
        height = tile

    staged = pl.pallas_call(
        stage_kernel,
        out_shape=jax.ShapeDtypeStruct(right.shape, right.dtype),
        in_specs=[pl.BlockSpec(memory_space=pltpu.HBM)],
        out_specs=VMEM,
        scratch_shapes=[pltpu.SemaphoreType.DMA((column_blocks,))],
        compiler_params=limits(8),
        name="stage",
    )(right)
    exchanged = []
    for at, ((picked, half), (arrays, spans)) in enumerate(zip(chunks, gathered)):
        tall = height * len(picked)
        part = tall // n_row
        own, *sent = pl.pallas_call(
            functools.partial(product_kernel, n_row, spans, half),
            out_shape=[jax.ShapeDtypeStruct((column_blocks, part, tile), jnp.float32)]
            + [jax.ShapeDtypeStruct((column_blocks * part + CODE_ROWS, tile), jnp.int16)] * (n_row - 1),
            in_specs=[SMEM] * 2 + [VMEM] * (len(arrays) + 1),
            out_specs=[VMEM] * n_row,
            scratch_shapes=[
                pltpu.VMEM((kept + 1, tall, tile), left_tiles.dtype),
                pltpu.VMEM((tall, tile), jnp.float32),
            ],
            cost_estimate=pl.CostEstimate(
                flops=2 * column_blocks * slots * tall * tile**2,
                bytes_accessed=right.size * 2,
                transcendentals=0,
            ),
            compiler_params=limits(16),
            name="product",
        )(right_index, right_count, *arrays, staged)
        got = [
            move(x, ("row", "col"), row_pairs(n_row, n_col, k, half), at)
            for k, x in enumerate(sent, 1)
        ]
        exchanged.append((own, got))
    squared, sums = [], None
    for at, (own, got) in enumerate(exchanged):
        square, sums = pl.pallas_call(
            functools.partial(reduce_kernel, n_row, at > 0),
            out_shape=[
                jax.ShapeDtypeStruct(own.shape, jnp.float32),
                jax.ShapeDtypeStruct((column_blocks, tile), jnp.float32),
            ],
            in_specs=[VMEM] * (n_row + (at > 0)),
            out_specs=[VMEM] * 2,
            compiler_params=limits(8),
            name="reduce",
        )(*got, own, *([sums] if at else []))
        squared.append(square)
    others = [move(sums, "row", [(i, i ^ k) for i in range(n_row)]) for k in range(1, n_row)]
    return pl.pallas_call(
        functools.partial(scale_kernel, chunks, n_row),
        out_shape=jax.ShapeDtypeStruct((windows, column_blocks, tile // n_row, tile), jnp.bfloat16),
        in_specs=[VMEM] * (len(chunks) + n_row),
        out_specs=VMEM,
        compiler_params=limits(8),
        name="scale",
    )(*squared, sums, *others)


def solution(mesh):
    in_specs = (
        P(None, "row", "col", None),
        P("col", "row", None, None),
        P("col", "row"),
        P("col", "row"),
    )
    out_specs = P(None, "col", "row", None)
    n_row, n_col = mesh.shape["row"], mesh.shape["col"]

    def body(*args):
        return shards(n_row, n_col, *args)

    return jax.shard_map(body, mesh=mesh, in_specs=in_specs, out_specs=out_specs, check_vma=False)
```

```python
import functools
import jax
import jax.numpy as jnp
from jax import lax
from jax.experimental import pallas as pl
from jax.experimental.pallas import tpu as pltpu
from jax.sharding import PartitionSpec as P


LEVELS = 65280.0
OFFSET = 32640
LOG_STEPS = 256.0
CODE_ROWS = 16
LINE = 4

VMEM = pl.BlockSpec(memory_space=pltpu.VMEM)
SMEM = pl.BlockSpec(memory_space=pltpu.SMEM)


def stage_kernel(index_ref, count_ref, right_ref, out_ref):
    column_blocks, slots = index_ref.shape
    out_ref[...] = jnp.zeros_like(out_ref)
    for j in range(column_blocks):
        for q in range(slots):

            def put(j=j, q=q):
                out_ref[j, index_ref[j, q]] = right_ref[j, q]

            pl.when(q < count_ref[j])(put)


def far_half(half):
    chip = lax.axis_index("col") >> 1
    return jnp.where(lax.axis_index("row") == chip ^ (LINE - 1), 1 - half, half)


def turned(k, half):
    if half is None or k > 2:
        return k
    return jnp.where(lax.axis_index("col") & 1 == 0, k, 3 - k)


def product_kernel(n_row, spans, half, *refs):
    n_block = len(refs) - n_row - 3
    blocks, right_ref, own_ref = refs[:n_block], refs[n_block], refs[n_block + 1]
    sent_refs = refs[n_block + 2 : n_block + 1 + n_row]
    left, partial = refs[-2:]
    column_blocks, kept, tile, _ = right_ref.shape
    height = left.shape[1]
    part = height // n_row // len(spans[0])
    row = lax.axis_index("row")

    def rows_of(owner, at):
        return pl.ds(pl.multiple_of((at * n_row + owner) * part, part), part)

    def block_of(span):
        at, a = span
        return blocks[at] if a is None else blocks[at].at[a]

    if half is None:
        left[...] = block_of(spans[0][0])[...]
    else:
        core, chip = lax.axis_index("col") & 1, lax.axis_index("col") >> 1
        ends = (chip == 0) | (chip == LINE - 1)
        first, last = core == 0, core == 1
        placed = [(half, 0, first), (1 - half, 0, last)]
        placed += [(2 + half, 1, first), (3 - half, 1, last), (4, 2, first), (5, 2, last)]
        if half:
            inner = jnp.logical_not(ends)
            placed += [(5, 3, first & inner), (4, 3, last & inner)]
            placed += [(7, 3, first & ends), (6, 3, last & ends)]
        else:
            placed += [(5, 3, first), (4, 3, last)]
        for role, k, wanted in placed:

            def fill(role=role, k=k):
                for at, span in enumerate(spans[role]):
                    left[:, rows_of(chip ^ k, at), :] = block_of(span)[...]

            pl.when(wanted)(fill)
    lines = lax.broadcasted_iota(jnp.int32, (CODE_ROWS, tile), 0)
    codes = jnp.zeros((CODE_ROWS, tile), jnp.int32)
    count = len(spans[0])
    for j in range(column_blocks):
        total = None
        for k in range(kept):
            term = jnp.dot(left[k], right_ref[j, k], preferred_element_type=jnp.float32)
            total = term if total is None else total + term
        partial[...] = total
        top = jnp.max(total, axis=0, keepdims=True)
        code = jnp.floor(jnp.log2(top) * LOG_STEPS).astype(jnp.int32) + 2
        grow = LEVELS * jnp.exp2(code.astype(jnp.float32) * (-1.0 / LOG_STEPS))
        codes = jnp.where(lines == j, code, codes)
        for at in range(count):
            own_ref[j, at * part : (at + 1) * part, :] = partial[rows_of(row, at), :]
            for k in range(1, n_row):
                coded = (partial[rows_of(row ^ turned(k, half), at), :] * grow + 0.5).astype(jnp.int32) - OFFSET
                first = (j * count + at) * part
                sent_refs[k - 1][first : first + part, :] = coded.astype(jnp.int16)
    for sent in sent_refs:
        sent[column_blocks * count * part :, :] = codes.astype(jnp.int16)


def reduce_kernel(n_row, has_before, *refs):
    got_refs = refs[: n_row - 1]
    own_ref = refs[n_row - 1]
    before_ref = refs[n_row] if has_before else None
    squared_ref, sums_ref = refs[-2:]
    column_blocks, part, _ = own_ref.shape
    shrinks = []
    for got in got_refs:
        code = got[column_blocks * part :, :].astype(jnp.int32)
        shrinks.append(jnp.exp2(code.astype(jnp.float32) * (1.0 / LOG_STEPS)) * (1.0 / LEVELS))
    for j in range(column_blocks):
        total = own_ref[j]
        for got, shrink in zip(got_refs, shrinks):
            coded = got[j * part : (j + 1) * part, :].astype(jnp.int32) + OFFSET
            total = total + coded.astype(jnp.float32) * shrink[j : j + 1]
        squared = total * total
        squared_ref[j] = squared
        sums = jnp.sum(squared, axis=0, keepdims=True)
        if has_before:
            sums = sums + before_ref[j : j + 1]
        sums_ref[j : j + 1] = sums


def scale_kernel(chunks, n_row, *refs):
    squared_refs = refs[: len(chunks)]
    sums_refs = refs[len(chunks) : len(chunks) + n_row]
    out_ref = refs[-1]
    windows, column_blocks, _, tile = out_ref.shape
    total = sums_refs[0][...]
    for other in sums_refs[1:]:
        total = total + other[...]
    scale = (windows * tile) / total
    for (picked, half), squared in zip(chunks, squared_refs):
        rows = squared.shape[1] // len(picked)
        for at, a in enumerate(picked):
            for j in range(column_blocks):
                value = squared[j, at * rows : (at + 1) * rows, :] * scale[j : j + 1]
                first = 0 if half is None else pl.multiple_of(far_half(half) * rows, rows)
                out_ref[a, j, pl.ds(first, rows), :] = value.astype(out_ref.dtype)


def move(x, axis, pairs, turn=0):
    return lax.ppermute(x, axis, pairs[turn:] + pairs[:turn])


def row_pairs(n_row, n_col, k, half):
    pairs = []
    for i in range(n_row * n_col):
        row, col = i // n_col, i % n_col
        peer = 3 - k if half is not None and k < 3 and col & 1 else k
        pairs.append((i, (row ^ peer) * n_col + col))
    return pairs


def limits(mib):
    return pltpu.CompilerParams(vmem_limit_bytes=mib << 20)


def is_line(n_row, n_col):
    return n_row == LINE and n_col == 2 * LINE


def gather_line(left_tiles, n_col):
    windows = left_tiles.shape[0]
    swap = [(i, i ^ 1) for i in range(n_col)]
    across = [(i, i ^ (4 if i & 1 == 0 else 6)) for i in range(n_col)]
    inner = [p if p[0] & 1 == 0 or 2 <= p[0] < n_col - 2 else (p[0], p[0]) for p in across]
    beside = move(left_tiles, "col", [(i, i ^ 2) for i in range(n_col)])
    own = move(left_tiles, "col", across)
    pair = move(left_tiles, "col", swap, 1)
    other = move(pair, "col", inner)
    relay = move(own, "col", [(2, 1), (n_col - 4, n_col - 1)])
    near_beside = move(beside, "col", swap, 2)
    near_own = move(own, "col", swap, 3)
    near_other = move(other, "col", swap, 4)
    near_relay = move(relay, "col", swap, 5)
    base = [left_tiles, pair, beside, near_beside]
    chunks, gathered = [], []
    for half, more in enumerate(([own, near_own], [other, near_other, relay, near_relay])):
        arrays = base + more
        chunks.append((tuple(range(windows)), half))
        gathered.append((arrays, tuple(tuple((at, a) for a in range(windows)) for at in range(len(arrays)))))
    return chunks, gathered


def shards(n_row, n_col, left_tiles, right, right_index, right_count):
    windows, kept, _, tile = left_tiles.shape
    column_blocks = right.shape[0]
    right_count = right_count.reshape(-1)

    if is_line(n_row, n_col):
        chunks, gathered = gather_line(left_tiles, n_col)
        height = tile // 2
    else:
        whole = lax.all_gather(left_tiles, "col", axis=2, tiled=True)
        chunks = [((a,), None) for a in range(windows)]
        gathered = [([whole], (((0, a),),)) for a in range(windows)]
        height = tile

    staged = pl.pallas_call(
        stage_kernel,
        out_shape=jax.ShapeDtypeStruct((column_blocks, kept, tile, tile), right.dtype),
        in_specs=[SMEM] * 2 + [VMEM],
        out_specs=VMEM,
        compiler_params=limits(8),
        name="stage",
    )(right_index, right_count, right)
    exchanged = []
    for at, ((picked, half), (arrays, spans)) in enumerate(zip(chunks, gathered)):
        tall = height * len(picked)
        part = tall // n_row
        own, *sent = pl.pallas_call(
            functools.partial(product_kernel, n_row, spans, half),
            out_shape=[jax.ShapeDtypeStruct((column_blocks, part, tile), jnp.float32)]
            + [jax.ShapeDtypeStruct((column_blocks * part + CODE_ROWS, tile), jnp.int16)] * (n_row - 1),
            in_specs=[VMEM] * (len(arrays) + 1),
            out_specs=[VMEM] * n_row,
            scratch_shapes=[
                pltpu.VMEM((kept, tall, tile), left_tiles.dtype),
                pltpu.VMEM((tall, tile), jnp.float32),
            ],
            cost_estimate=pl.CostEstimate(
                flops=2 * column_blocks * kept * tall * tile**2,
                bytes_accessed=right.size * 2,
                transcendentals=0,
            ),
            compiler_params=limits(16),
            name="product",
        )(*arrays, staged)
        got = [
            move(x, ("row", "col"), row_pairs(n_row, n_col, k, half), at)
            for k, x in enumerate(sent, 1)
        ]
        exchanged.append((own, got))
    squared, sums = [], None
    for at, (own, got) in enumerate(exchanged):
        square, sums = pl.pallas_call(
            functools.partial(reduce_kernel, n_row, at > 0),
            out_shape=[
                jax.ShapeDtypeStruct(own.shape, jnp.float32),
                jax.ShapeDtypeStruct((column_blocks, tile), jnp.float32),
            ],
            in_specs=[VMEM] * (n_row + (at > 0)),
            out_specs=[VMEM] * 2,
            compiler_params=limits(8),
            name="reduce",
        )(*got, own, *([sums] if at else []))
        squared.append(square)
    others = [move(sums, "row", [(i, i ^ k) for i in range(n_row)]) for k in range(1, n_row)]
    return pl.pallas_call(
        functools.partial(scale_kernel, chunks, n_row),
        out_shape=jax.ShapeDtypeStruct((windows, column_blocks, tile // n_row, tile), jnp.bfloat16),
        in_specs=[VMEM] * (len(chunks) + n_row),
        out_specs=VMEM,
        compiler_params=limits(8),
        name="scale",
    )(*squared, sums, *others)


def solution(mesh):
    in_specs = (
        P(None, "row", "col", None),
        P("col", "row", None, None),
        P("col", "row"),
        P("col", "row"),
    )
    out_specs = P(None, "col", "row", None)
    n_row, n_col = mesh.shape["row"], mesh.shape["col"]

    def body(*args):
        return shards(n_row, n_col, *args)

    return jax.shard_map(body, mesh=mesh, in_specs=in_specs, out_specs=out_specs, check_vma=False)
```

```python
import functools
import jax
import jax.numpy as jnp
from jax import lax
from jax.experimental import pallas as pl
from jax.experimental.pallas import tpu as pltpu
from jax.sharding import PartitionSpec as P


LEVELS = 65280.0
OFFSET = 32640
LOG_STEPS = 256.0
CODE_ROWS = 8
LINE = 4

VMEM = pl.BlockSpec(memory_space=pltpu.VMEM)
SMEM = pl.BlockSpec(memory_space=pltpu.SMEM)


def stage_kernel(index_ref, count_ref, right_ref, out_ref):
    column_blocks, slots = index_ref.shape
    out_ref[...] = jnp.zeros_like(out_ref)
    for j in range(column_blocks):
        for q in range(slots):

            def put(j=j, q=q):
                out_ref[j, index_ref[j, q]] = right_ref[j, q]

            pl.when(q < count_ref[j])(put)


def far_half(half):
    chip = lax.axis_index("col") >> 1
    return jnp.where(lax.axis_index("row") == chip ^ (LINE - 1), 1 - half, half)


def turned(k, half):
    if half is None or k > 2:
        return k
    return jnp.where(lax.axis_index("col") & 1 == 0, k, 3 - k)


def product_kernel(n_row, spans, half, *refs):
    n_block = len(refs) - n_row - 3
    blocks, right_ref, own_ref = refs[:n_block], refs[n_block], refs[n_block + 1]
    sent_refs = refs[n_block + 2 : n_block + 1 + n_row]
    left, partial = refs[-2:]
    column_blocks, kept, tile, _ = right_ref.shape
    height = left.shape[1]
    part = height // n_row // len(spans[0])
    row = lax.axis_index("row")

    def rows_of(owner, at):
        return pl.ds(pl.multiple_of((at * n_row + owner) * part, part), part)

    def block_of(span):
        at, a = span
        return blocks[at] if a is None else blocks[at].at[a]

    if half is None:
        left[...] = block_of(spans[0][0])[...]
    else:
        core, chip = lax.axis_index("col") & 1, lax.axis_index("col") >> 1
        ends = (chip == 0) | (chip == LINE - 1)
        first, last = core == 0, core == 1
        placed = [(half, 0, first), (1 - half, 0, last)]
        placed += [(2 + half, 1, first), (3 - half, 1, last), (4, 2, first), (5, 2, last)]
        if half:
            inner = jnp.logical_not(ends)
            placed += [(5, 3, first & inner), (4, 3, last & inner)]
            placed += [(7, 3, first & ends), (6, 3, last & ends)]
        else:
            placed += [(5, 3, first), (4, 3, last)]
        for role, k, wanted in placed:

            def fill(role=role, k=k):
                for at, span in enumerate(spans[role]):
                    left[:, rows_of(chip ^ k, at), :] = block_of(span)[...]

            pl.when(wanted)(fill)
    lines = lax.broadcasted_iota(jnp.int32, (CODE_ROWS, tile), 0)
    codes = jnp.zeros((CODE_ROWS, tile), jnp.int32)
    count = len(spans[0])
    for j in range(column_blocks):
        total = None
        for k in range(kept):
            term = jnp.dot(left[k], right_ref[j, k], preferred_element_type=jnp.float32)
            total = term if total is None else total + term
        partial[...] = total
        top = jnp.max(total, axis=0, keepdims=True)
        code = jnp.floor(jnp.log2(top) * LOG_STEPS).astype(jnp.int32) + 2
        grow = LEVELS * jnp.exp2(code.astype(jnp.float32) * (-1.0 / LOG_STEPS))
        codes = jnp.where(lines == j, code, codes)
        for at in range(count):
            own_ref[j, at * part : (at + 1) * part, :] = partial[rows_of(row, at), :]
            for k in range(1, n_row):
                coded = (partial[rows_of(row ^ turned(k, half), at), :] * grow + 0.5).astype(jnp.int32) - OFFSET
                first = (j * count + at) * part
                sent_refs[k - 1][first : first + part, :] = coded.astype(jnp.int16)
    for sent in sent_refs:
        sent[column_blocks * count * part :, :] = codes.astype(jnp.int16)


def reduce_kernel(n_row, has_before, *refs):
    got_refs = refs[: n_row - 1]
    own_ref = refs[n_row - 1]
    before_ref = refs[n_row] if has_before else None
    squared_ref, sums_ref = refs[-2:]
    column_blocks, part, _ = own_ref.shape
    shrinks = []
    for got in got_refs:
        code = got[column_blocks * part :, :].astype(jnp.int32)
        shrinks.append(jnp.exp2(code.astype(jnp.float32) * (1.0 / LOG_STEPS)) * (1.0 / LEVELS))
    for j in range(column_blocks):
        total = own_ref[j]
        for got, shrink in zip(got_refs, shrinks):
            coded = got[j * part : (j + 1) * part, :].astype(jnp.int32) + OFFSET
            total = total + coded.astype(jnp.float32) * shrink[j : j + 1]
        squared = total * total
        squared_ref[j] = squared
        sums = jnp.sum(squared, axis=0, keepdims=True)
        if has_before:
            sums = sums + before_ref[j : j + 1]
        sums_ref[j : j + 1] = sums


def scale_kernel(chunks, n_row, *refs):
    squared_refs = refs[: len(chunks)]
    sums_refs = refs[len(chunks) : len(chunks) + n_row]
    out_ref = refs[-1]
    windows, column_blocks, _, tile = out_ref.shape
    total = sums_refs[0][...]
    for other in sums_refs[1:]:
        total = total + other[...]
    scale = (windows * tile) / total
    for (picked, half), squared in zip(chunks, squared_refs):
        rows = squared.shape[1] // len(picked)
        for at, a in enumerate(picked):
            for j in range(column_blocks):
                value = squared[j, at * rows : (at + 1) * rows, :] * scale[j : j + 1]
                first = 0 if half is None else pl.multiple_of(far_half(half) * rows, rows)
                out_ref[a, j, pl.ds(first, rows), :] = value.astype(out_ref.dtype)


def move(x, axis, pairs, turn=0):
    return lax.ppermute(x, axis, pairs[turn:] + pairs[:turn])


def row_pairs(n_row, n_col, k, half):
    pairs = []
    for i in range(n_row * n_col):
        row, col = i // n_col, i % n_col
        peer = 3 - k if half is not None and k < 3 and col & 1 else k
        pairs.append((i, (row ^ peer) * n_col + col))
    return pairs


def limits(mib):
    return pltpu.CompilerParams(vmem_limit_bytes=mib << 20)


def is_line(n_row, n_col):
    return n_row == LINE and n_col == 2 * LINE


def gather_line(left_tiles, n_col):
    windows = left_tiles.shape[0]
    swap = [(i, i ^ 1) for i in range(n_col)]
    across = [(i, i ^ (4 if i & 1 == 0 else 6)) for i in range(n_col)]
    inner = [p if p[0] & 1 == 0 or 2 <= p[0] < n_col - 2 else (p[0], p[0]) for p in across]
    beside = move(left_tiles, "col", [(i, i ^ 2) for i in range(n_col)])
    own = move(left_tiles, "col", across)
    pair = move(left_tiles, "col", swap, 1)
    other = move(pair, "col", inner)
    relay = move(own, "col", [(2, 1), (n_col - 4, n_col - 1)])
    near_beside = move(beside, "col", swap, 2)
    near_own = move(own, "col", swap, 2)
    near_other = move(other, "col", swap, 4)
    near_relay = move(relay, "col", swap, 4)
    base = [left_tiles, pair, beside, near_beside]
    chunks, gathered = [], []
    for half, more in enumerate(([own, near_own], [other, near_other, relay, near_relay])):
        arrays = base + more
        chunks.append((tuple(range(windows)), half))
        gathered.append((arrays, tuple(tuple((at, a) for a in range(windows)) for at in range(len(arrays)))))
    return chunks, gathered


def shards(n_row, n_col, left_tiles, right, right_index, right_count):
    windows, kept, _, tile = left_tiles.shape
    column_blocks = right.shape[0]
    right_count = right_count.reshape(-1)

    if is_line(n_row, n_col):
        chunks, gathered = gather_line(left_tiles, n_col)
        height = tile // 2
    else:
        whole = lax.all_gather(left_tiles, "col", axis=2, tiled=True)
        chunks = [((a,), None) for a in range(windows)]
        gathered = [([whole], (((0, a),),)) for a in range(windows)]
        height = tile

    staged = pl.pallas_call(
        stage_kernel,
        out_shape=jax.ShapeDtypeStruct((column_blocks, kept, tile, tile), right.dtype),
        in_specs=[SMEM] * 2 + [VMEM],
        out_specs=VMEM,
        compiler_params=limits(8),
        name="stage",
    )(right_index, right_count, right)
    exchanged = []
    for at, ((picked, half), (arrays, spans)) in enumerate(zip(chunks, gathered)):
        tall = height * len(picked)
        part = tall // n_row
        own, *sent = pl.pallas_call(
            functools.partial(product_kernel, n_row, spans, half),
            out_shape=[jax.ShapeDtypeStruct((column_blocks, part, tile), jnp.float32)]
            + [jax.ShapeDtypeStruct((column_blocks * part + CODE_ROWS, tile), jnp.int16)] * (n_row - 1),
            in_specs=[VMEM] * (len(arrays) + 1),
            out_specs=[VMEM] * n_row,
            scratch_shapes=[
                pltpu.VMEM((kept, tall, tile), left_tiles.dtype),
                pltpu.VMEM((tall, tile), jnp.float32),
            ],
            cost_estimate=pl.CostEstimate(
                flops=2 * column_blocks * kept * tall * tile**2,
                bytes_accessed=right.size * 2,
                transcendentals=0,
            ),
            compiler_params=limits(16),
            name="product",
        )(*arrays, staged)
        got = [
            move(x, ("row", "col"), row_pairs(n_row, n_col, k, half), at)
            for k, x in enumerate(sent, 1)
        ]
        exchanged.append((own, got))
    squared, sums = [], None
    for at, (own, got) in enumerate(exchanged):
        square, sums = pl.pallas_call(
            functools.partial(reduce_kernel, n_row, at > 0),
            out_shape=[
                jax.ShapeDtypeStruct(own.shape, jnp.float32),
                jax.ShapeDtypeStruct((column_blocks, tile), jnp.float32),
            ],
            in_specs=[VMEM] * (n_row + (at > 0)),
            out_specs=[VMEM] * 2,
            compiler_params=limits(8),
            name="reduce",
        )(*got, own, *([sums] if at else []))
        squared.append(square)
    others = [move(sums, "row", [(i, i ^ k) for i in range(n_row)]) for k in range(1, n_row)]
    return pl.pallas_call(
        functools.partial(scale_kernel, chunks, n_row),
        out_shape=jax.ShapeDtypeStruct((windows, column_blocks, tile // n_row, tile), jnp.bfloat16),
        in_specs=[VMEM] * (len(chunks) + n_row),
        out_specs=VMEM,
        compiler_params=limits(8),
        name="scale",
    )(*squared, sums, *others)


def solution(mesh):
    in_specs = (
        P(None, "row", "col", None),
        P("col", "row", None, None),
        P("col", "row"),
        P("col", "row"),
    )
    out_specs = P(None, "col", "row", None)
    n_row, n_col = mesh.shape["row"], mesh.shape["col"]

    def body(*args):
        return shards(n_row, n_col, *args)

    return jax.shard_map(body, mesh=mesh, in_specs=in_specs, out_specs=out_specs, check_vma=False)
```
